32 devices in a mesh: blk: 8 (over y, x, core), grp: 4 (over z).
Axes of the slice: x: 2, y: 2, z: 4, core: 2. Of those that a mesh axis runs over, the one named last changes fastest.
Arguments:
- image_embeds: bfloat16 [4096, 1152], P(('blk', 'grp')), may hold values from -6 to 6
- text_embeds: bfloat16 [4096, 1152], P(('blk', 'grp')), may hold values from -6 to 6
Outputs:
- image_embed_gradient: bfloat16 [4096, 1152], P(('blk', 'grp'))
- text_embed_gradient: bfloat16 [4096, 1152], P(('blk', 'grp'))
The draws below stay inside these ranges and needn't reach their ends.
All inputs are finite; a program needn't handle non-finite values.
Results may differ from the reference program's by a relative error of at most 0.0059.
Values may be sent and summed in bfloat16 or wider, within the bound.
A program may use at most 64 MiB of HBM per device.

```python
import jax
import jax.numpy as jnp
from jax import lax

EMBED_WIDTH = 1152
BLOCK_ROWS = 128
STEPS = 16
BATCH = 4096


def block_scale(rng, dims, cuts, smallest, largest):
    def one(position, blocks):
        heights = jax.random.uniform(jax.random.fold_in(jax.random.fold_in(rng, 6), position), (blocks,), jnp.float32, smallest / len(cuts), largest / len(cuts))
        return jnp.repeat(jnp.exp(heights), dims[position] // blocks).reshape((-1,) + (1,) * (len(dims) - position - 1))

    loudness = one(*cuts[0])
    for cut in cuts[1:]:
        loudness = loudness * one(*cut)
    return loudness


def gaussian(key, extent, scale, reach, split=(), held_as=jnp.bfloat16):
    drawn = scale * jax.random.normal(key, extent, jnp.float32)
    if split:
        drawn = drawn * block_scale(key, extent, split, -0.22, 0.18)
    return jnp.clip(drawn, -reach, reach).astype(held_as)


def setup_inputs(seed: int = 0) -> dict:
    seeds = jax.random.split(jax.random.key(seed), 3)
    return {
        "image_embeds": gaussian(seeds[0], (BATCH, EMBED_WIDTH), 1.0, 6.0, ((0, 32),)),
        "text_embeds": gaussian(seeds[1], (BATCH, EMBED_WIDTH), 1.0, 6.0, ((0, 32),)),
    }


LOGIT_SCALE = 10.0
BIAS_LOGIT = -2.0
EPSILON = 1e-06

def normalize(values):
    wide = values.astype(jnp.float32)
    length = jnp.sqrt(lax.optimization_barrier(jnp.sum(wide * wide, axis=-1, keepdims=True)) + EPSILON)
    return (wide / length, length)

def undo_normalization(grad, unit, length):
    inner = lax.optimization_barrier(jnp.sum(unit * grad, axis=-1, keepdims=True))
    return (grad - unit * inner) / length

def pair_weights(pair_logits, is_first):
    count = pair_logits.shape[-1]
    diagonal_mask = jnp.eye(count, dtype=bool) & is_first
    return jnp.where(diagonal_mask, -jax.nn.sigmoid(-pair_logits), jax.nn.sigmoid(pair_logits))

def reference(image_embeds, text_embeds):
    block_list = image_embeds.shape[0] // BLOCK_ROWS
    image_normalized, image_norm = normalize(image_embeds)
    text_normalized, text_norm = normalize(text_embeds)
    image_reduced = image_normalized.astype(jnp.bfloat16).astype(jnp.float32).reshape(block_list, BLOCK_ROWS, EMBED_WIDTH)
    text_low = text_normalized.astype(jnp.bfloat16).astype(jnp.float32).reshape(block_list, BLOCK_ROWS, EMBED_WIDTH)

    def advance(running, offset):
        image_total, text_total = running
        shifted_block = jnp.roll(text_low, offset, axis=0)
        pair_logits = LOGIT_SCALE * jnp.einsum('gty,gky->gtk', image_reduced, shifted_block) + BIAS_LOGIT
        weights = pair_weights(pair_logits, offset == 0).astype(jnp.bfloat16).astype(jnp.float32)
        image_total = image_total + jnp.einsum('prc,pcd->prd', weights, shifted_block)
        text_terms = jnp.einsum('prc,prd->pcd', weights, image_reduced)
        text_total = text_total + jnp.roll(text_terms, -offset, axis=0)
        return ((image_total, text_total), None)
    zeros = jnp.zeros((block_list, BLOCK_ROWS, EMBED_WIDTH), jnp.float32)
    (image_total, text_total), _ = lax.scan(advance, (zeros, zeros), jnp.arange(STEPS, dtype=jnp.int32))
    image_gradient = LOGIT_SCALE * image_total.reshape(block_list * BLOCK_ROWS, EMBED_WIDTH)
    text_gradient = LOGIT_SCALE * text_total.reshape(block_list * BLOCK_ROWS, EMBED_WIDTH)
    image_embed_gradient = undo_normalization(image_gradient, image_normalized, image_norm).astype(jnp.bfloat16)
    text_embed_gradient = undo_normalization(text_gradient, text_normalized, text_norm).astype(jnp.bfloat16)
    return (image_embed_gradient, text_embed_gradient)
```

```python
import functools

import jax
import jax.numpy as jnp
from jax import lax
from jax.experimental import pallas as pl
from jax.experimental.pallas import tpu as pltpu
from jax.sharding import PartitionSpec as P

LOGIT_SCALE = 10.0
BIAS_LOGIT = -2.0
EPSILON = 1e-06
MESH = pl.DeviceIdType.MESH


def kernel(chips, depth, reach, window, image_ref, text_ref, image_out, text_out,
           held, total, own_scale, local_sem, send_sem, recv_sem):
    blk = lax.axis_index("blk")
    grp = lax.axis_index("grp")
    chip, core = blk // 2, blk % 2
    relayed = chips == 4 and reach == 2
    slots = 2 * (reach + 1)

    def view(kind):
        if kind == 0:
            return chip, core, grp
        return chips - 1 - chip, 1 - core, depth - 1 - grp

    def device(kind, c, k, z):
        c = (c + chips) % chips
        if kind == 0:
            return (2 * c + k, z)
        return (2 * (chips - 1 - c) + 1 - k, depth - 1 - z)

    def need(k, z, d, source_k, source_z):
        offset = (2 * d + k - source_k) * depth + z - source_z
        return (offset >= 0) & (offset < window)

    def chip_need(z, d, source_k, source_z):
        return need(0, z, d, source_k, source_z) | need(1, z, d, source_k, source_z)

    def arrives(kind, d, source_z):
        c, k, z = view(kind)
        wanted = chip_need(z, d, k, source_z)
        if relayed and d == 2:
            wanted = wanted | ((c % 2 == 1) & chip_need(z, 1, k, source_z))
        return wanted

    def copy(kind, path, source_slot, target_slot, z, target):
        return pltpu.make_async_remote_copy(
            src_ref=held.at[kind, source_slot, z],
            dst_ref=held.at[kind, target_slot, z],
            send_sem=send_sem.at[kind, path, z],
            recv_sem=recv_sem.at[kind, target_slot, z],
            device_id=target,
            device_id_type=MESH,
        )

    def own_sends(kind, z2):
        c, k, z = view(kind)
        sends = [
            ((z2 <= z) & (z + 1 < depth), 0, k, k, (c, k, z + 1)),
            ((z2 >= z) & (z >= 1), 1, k, k, (c, k, z - 1)),
        ]
        for d in range(1, reach + 1):
            wanted = chip_need(z, d, k, z2)
            if relayed and d == 1:
                wanted = wanted & (c % 2 == 0)
            if relayed and d == 2:
                wanted = wanted | ((c % 2 == 1) & chip_need(z, 1, k, z2))
            sends.append((wanted, 1 + d, k, 2 * d + k, (c + d, k, z)))
        sends.append((need(1 - k, z, 0, k, z2), 2 + reach, k, k, (c, 1 - k, z)))
        return sends

    def arrival_sends(kind, d, z2):
        c, k, z = view(kind)
        sends = []
        if relayed and d == 2:
            sends.append(((c % 2 == 1) & chip_need(z, 1, k, z2),
                          3 + reach, 4 + k, 2 + k, (c - 1, k, z)))
        sends.append((need(1 - k, z, d, k, z2), 3 + reach + d, 2 * d + k, 2 * d + k, (c, 1 - k, z)))
        return sends

    def each(kind, sends, z2, finish=False):
        for wanted, path, source_slot, target_slot, target in sends:
            @pl.when(wanted)
            def _():
                moved = copy(kind, path, source_slot, target_slot, z2, device(kind, *target))
                if finish:
                    moved.wait_send()
                else:
                    moved.start()

    def await_block(kind, slot, z2):
        c, k, z = view(kind)
        copy(kind, 0, slot, slot, z2, device(kind, c, 1 - k, z)).wait_recv()

    own = []
    for kind, ref in ((0, text_ref), (1, image_ref)):
        _, k, z = view(kind)
        loaded = pltpu.make_async_copy(ref, held.at[kind, k, z], local_sem.at[kind])
        loaded.start()
        own.append(loaded)

    barrier = pltpu.get_barrier_semaphore()

    def greet(target):
        pl.semaphore_signal(barrier, inc=1, device_id=target, device_id_type=MESH)

    greet((2 * chip + 1 - core, grp))
    if relayed:
        partners = [chip + 1 - 2 * (chip % 2), (chip + 2) % 4]
    else:
        partners = [(chip + d + chips) % chips for d in range(-reach, reach + 1) if d]
    for partner in partners:
        greet((2 * partner + core, grp))

    @pl.when(grp > 0)
    def _():
        greet((blk, grp - 1))

    @pl.when(grp < depth - 1)
    def _():
        greet((blk, grp + 1))

    for loaded in own:
        loaded.wait()
    pl.semaphore_wait(
        barrier,
        1 + len(partners) + (grp > 0).astype(jnp.int32) + (grp < depth - 1).astype(jnp.int32),
    )

    def views(kind):
        k = jnp.where(kind == 0, core, 1 - core)
        z = jnp.where(kind == 0, grp, depth - 1 - grp)
        return k, z

    def own_block(kind):
        k, z = views(kind)
        return held[kind, k, z]

    def inverse_length(block):
        wide = block.astype(jnp.float32)
        return lax.rsqrt(jnp.sum(wide * wide, axis=-1, keepdims=True) + EPSILON)

    rows = held.shape[3]

    def tile(kind, slot, z2):
        k, z = views(kind)
        other = held[kind, slot, z2]
        mine = own_block(1 - kind)
        columns = jnp.broadcast_to(inverse_length(other), (rows, rows)).T
        product = lax.dot_general(
            mine, other, (((1,), (1,)), ((), ())), preferred_element_type=jnp.float32
        )
        logits = LOGIT_SCALE * product * own_scale[kind] * columns + BIAS_LOGIT
        inverse = jnp.exp(-logits)
        weights = 1.0 / (1.0 + inverse)
        diagonal = lax.broadcasted_iota(jnp.int32, (rows, rows), 0) == lax.broadcasted_iota(
            jnp.int32, (rows, rows), 1
        )
        first = ((slot == k) & (z2 == z)).astype(jnp.float32)
        positive = jnp.where(diagonal, first, 0.0)
        weights = jnp.where(positive > 0.5, -inverse * weights, weights)
        scaled = (weights * columns).astype(jnp.bfloat16)
        total[kind] += jnp.dot(scaled, other, preferred_element_type=jnp.float32)

    def position(kind, sign, distance):
        _, _, z = view(kind)
        z2 = z + sign * distance
        valid = (z2 >= 0) & (z2 < depth) & (distance >= 0)
        if sign < 0:
            valid = valid & (distance > 0)
        return z2, valid

    def advance(turn, carry):
        for kind in (0, 1):
            for sign in (1, -1):
                z2, valid = position(kind, sign, turn)

                @pl.when(valid)
                def _():
                    @pl.when(turn > 0)
                    def _():
                        await_block(kind, view(kind)[1], z2)

                    each(kind, own_sends(kind, z2), z2)

        @pl.when(turn == 0)
        def _():
            def prepare(kind, carry):
                total[kind] = jnp.zeros(total.shape[1:], jnp.float32)
                own_scale[kind] = jnp.broadcast_to(inverse_length(own_block(1 - kind)), (rows, rows))
                return carry

            lax.fori_loop(0, 2, prepare, 0)

        for d in range(reach, 0, -1):
            for kind in (0, 1):
                for sign in (1, -1):
                    z2, valid = position(kind, sign, turn - 1)

                    @pl.when(valid & arrives(kind, d, z2))
                    def _():
                        await_block(kind, 2 * d + view(kind)[1], z2)
                        each(kind, arrival_sends(kind, d, z2), z2)

        def work(index, carry):
            slot = index // 4
            kind = (index // 2) % 2
            sign = 1 - 2 * (index % 2)
            k, z = views(kind)
            z2 = z + sign * (turn - 1)
            d, source_k = slot // 2, slot % 2
            valid = (turn > 0) & (z2 >= 0) & (z2 < depth) & ((sign > 0) | (turn > 1))

            @pl.when(valid & need(k, z, d, source_k, z2))
            def _():
                @pl.when(source_k != k)
                def _():
                    pltpu.make_async_remote_copy(
                        src_ref=held.at[kind, slot, z2],
                        dst_ref=held.at[kind, slot, z2],
                        send_sem=send_sem.at[kind, 0, z2],
                        recv_sem=recv_sem.at[kind, slot, z2],
                        device_id=(2 * chip + 1 - core, grp),
                        device_id_type=MESH,
                    ).wait_recv()

                tile(kind, slot, z2)

            return carry

        lax.fori_loop(0, 4 * slots, work, 0)
        return carry

    lax.fori_loop(0, depth + 1, advance, 0)

    for kind, out in ((0, image_out), (1, text_out)):
        scale = own_scale[kind][:, :1]
        unit = own_block(1 - kind).astype(jnp.float32) * scale
        grad = LOGIT_SCALE * total[kind]
        inner = jnp.sum(unit * grad, axis=-1, keepdims=True)
        out[...] = ((grad - unit * inner) * scale).astype(out.dtype)

    def settle(z2, carry):
        for kind in (0, 1):
            each(kind, own_sends(kind, z2), z2, finish=True)
            for d in range(1, reach + 1):
                @pl.when(arrives(kind, d, z2))
                def _():
                    each(kind, arrival_sends(kind, d, z2), z2, finish=True)
        return carry

    lax.fori_loop(0, depth, settle, 0)


def solution(mesh):
    cycle, depth = mesh.shape["blk"], mesh.shape["grp"]
    window = min(20, cycle * depth // 2)
    chips = cycle // 2
    reach = 1
    while (2 * reach + 1) * depth - (depth - 1) < window:
        reach += 1
    slots = 2 * (reach + 1)

    def per_device(image_embeds, text_embeds):
        rows, width = image_embeds.shape
        shape = jax.ShapeDtypeStruct((rows, width), jnp.bfloat16)
        return pl.pallas_call(
            functools.partial(kernel, chips, depth, reach, window),
            out_shape=(shape, shape),
            in_specs=[pl.BlockSpec(memory_space=pl.ANY)] * 2,
            out_specs=(pl.BlockSpec(memory_space=pltpu.VMEM),) * 2,
            scratch_shapes=[
                pltpu.VMEM((2, slots, depth, rows, width), jnp.bfloat16),
                pltpu.VMEM((2, rows, width), jnp.float32),
                pltpu.VMEM((2, rows, rows), jnp.float32),
                pltpu.SemaphoreType.DMA((2,)),
                pltpu.SemaphoreType.DMA((2, 4 + 2 * reach, depth)),
                pltpu.SemaphoreType.DMA((2, slots, depth)),
            ],
            compiler_params=pltpu.CompilerParams(collective_id=0, has_side_effects=True),
        )(image_embeds, text_embeds)

    placed = P(("blk", "grp"), None)
    return jax.shard_map(
        per_device, mesh=mesh, in_specs=(placed, placed), out_specs=(placed, placed), check_vma=False
    )
```

```python
import functools

import jax
import jax.numpy as jnp
from jax import lax
from jax.experimental import pallas as pl
from jax.experimental.pallas import tpu as pltpu
from jax.sharding import PartitionSpec as P

LOGIT_SCALE = 10.0
BIAS_LOGIT = -2.0
EPSILON = 1e-06
MESH = pl.DeviceIdType.MESH


def kernel(chips, depth, reach, window, image_ref, text_ref, image_out, text_out,
           held, total, own_scale, local_sem, send_sem, recv_sem):
    blk = lax.axis_index("blk")
    grp = lax.axis_index("grp")
    chip, core = blk // 2, blk % 2
    relayed = chips == 4 and reach == 2 and 4 * depth - 1 < window

    def view(kind):
        return (
            chip + kind * (chips - 1 - 2 * chip),
            core + kind * (1 - 2 * core),
            grp + kind * (depth - 1 - 2 * grp),
        )

    def device(kind, c, k, z):
        c = (c + chips) % chips
        linear = 2 * c + k
        return (
            linear + kind * (2 * chips - 1 - 2 * linear),
            z + kind * (depth - 1 - 2 * z),
        )

    first_kind = 1 - chip % 2 if relayed else 0
    kinds = (first_kind, 1 - first_kind)

    def need(k, z, d, source_k, source_z):
        offset = (2 * d + k - source_k) * depth + z - source_z
        return (offset >= 0) & (offset < window)

    def chip_need(z, d, source_k, source_z):
        return need(0, z, d, source_k, source_z) | need(1, z, d, source_k, source_z)

    def arrives(kind, d, source_z):
        c, k, z = view(kind)
        wanted = chip_need(z, d, k, source_z)
        if relayed:
            wanted = wanted | ((d == 2) & (c % 2 == 1))
        return wanted

    def copy(kind, path, source_slot, target_slot, z, target):
        return pltpu.make_async_remote_copy(
            src_ref=held.at[kind, source_slot, z],
            dst_ref=held.at[kind, target_slot, z],
            send_sem=send_sem.at[kind, path, z],
            recv_sem=recv_sem.at[kind, target_slot, z],
            device_id=target,
            device_id_type=MESH,
        )

    def own_sends(kind, z2):
        c, k, z = view(kind)
        sends = [
            ((z2 <= z) & (z + 1 < depth), 0, k, k, (c, k, z + 1)),
            ((z2 >= z) & (z >= 1), 1, k, k, (c, k, z - 1)),
        ]
        for d in range(1, reach + 1):
            wanted = chip_need(z, d, k, z2)
            if relayed and d == 1:
                inside = (z2 > 0) & (z2 < depth - 1)
                wanted = (c % 2 == 0) & (inside | (z2 == z))
            if relayed and d == 2:
                wanted = wanted | (c % 2 == 1)
            sends.append((wanted, 1 + d, k, 2 * d + k, (c + d, k, z)))
        sends.append((need(1 - k, z, 0, k, z2), 2 + reach, k, k, (c, 1 - k, z)))
        return sends

    def arrival_sends(kind, d, z2):
        c, k, z = view(kind)
        sends = []
        slot = 2 * d + k
        if relayed:
            sends.append(((c % 2 == 1) & (d == 2), 3 + reach, slot, 2 + k, (c - 1, k, z)))
            outer = (c % 2 == 1) & (d == 1) & ((z2 == 0) | (z2 == depth - 1))
            sends.append((outer & (z2 <= z) & (z + 1 < depth),
                          4 + 2 * reach, slot, slot, (c, k, z + 1)))
            sends.append((outer & (z2 >= z) & (z >= 1),
                          5 + 2 * reach, slot, slot, (c, k, z - 1)))
        sends.append((need(1 - k, z, d, k, z2), 3 + reach + d, slot, slot, (c, 1 - k, z)))
        return sends

    def each(kind, sends, z2, finish=False):
        for wanted, path, source_slot, target_slot, target in sends:
            @pl.when(wanted)
            def _():
                moved = copy(kind, path, source_slot, target_slot, z2, device(kind, *target))
                if finish:
                    moved.wait_send()
                else:
                    moved.start()

    def await_block(kind, slot, z2):
        c, k, z = view(kind)
        copy(kind, 0, slot, slot, z2, device(kind, c, 1 - k, z)).wait_recv()

    own = []
    for kind, ref in ((0, text_ref), (1, image_ref)):
        _, k, z = view(kind)
        loaded = pltpu.make_async_copy(ref, held.at[kind, k, z], local_sem.at[kind])
        loaded.start()
        own.append(loaded)

    barrier = pltpu.get_barrier_semaphore()

    def greet(target):
        pl.semaphore_signal(barrier, inc=1, device_id=target, device_id_type=MESH)

    greet((2 * chip + 1 - core, grp))
    if relayed:
        partners = [chip + 1 - 2 * (chip % 2), (chip + 2) % 4]
    else:
        partners = [(chip + d + chips) % chips for d in range(-reach, reach + 1) if d]
    for partner in partners:
        greet((2 * partner + core, grp))

    @pl.when(grp > 0)
    def _():
        greet((blk, grp - 1))

    @pl.when(grp < depth - 1)
    def _():
        greet((blk, grp + 1))

    for loaded in own:
        loaded.wait()
    pl.semaphore_wait(
        barrier,
        1 + len(partners) + (grp > 0).astype(jnp.int32) + (grp < depth - 1).astype(jnp.int32),
    )

    def own_block(kind):
        _, k, z = view(kind)
        return held[kind, k, z]

    def inverse_length(block):
        wide = block.astype(jnp.float32)
        return lax.rsqrt(jnp.sum(wide * wide, axis=-1, keepdims=True) + EPSILON)

    rows = held.shape[3]

    def tile(kind, slot, z2):
        _, k, z = view(kind)
        other = held[kind, slot, z2]
        mine = own_block(1 - kind)
        columns = jnp.broadcast_to(inverse_length(other), (rows, rows)).T
        product = lax.dot_general(
            mine, other, (((1,), (1,)), ((), ())), preferred_element_type=jnp.float32
        )
        logits = LOGIT_SCALE * product * own_scale[kind] * columns + BIAS_LOGIT
        inverse = jnp.exp(-logits)
        weights = 1.0 / (1.0 + inverse)
        diagonal = lax.broadcasted_iota(jnp.int32, (rows, rows), 0) == lax.broadcasted_iota(
            jnp.int32, (rows, rows), 1
        )
        first = ((slot == k) & (z2 == z)).astype(jnp.float32)
        positive = jnp.where(diagonal, first, 0.0)
        weights = jnp.where(positive > 0.5, -inverse * weights, weights)
        scaled = (weights * columns).astype(jnp.bfloat16)
        total[kind] += jnp.dot(scaled, other, preferred_element_type=jnp.float32)

    def position(kind, sign, distance):
        _, _, z = view(kind)
        z2 = z + sign * distance
        valid = (z2 >= 0) & (z2 < depth) & (distance >= 0)
        return z2, valid & ((sign > 0) | (distance > 0))

    def advance(turn, carry):
        for kind in kinds:
            for sign in (1, -1):
                z2, valid = position(kind, sign, turn)

                @pl.when(valid)
                def _():
                    @pl.when(turn > 0)
                    def _():
                        await_block(kind, view(kind)[1], z2)

                    each(kind, own_sends(kind, z2), z2)

        @pl.when(turn == 0)
        def _():
            def prepare(kind, carry):
                total[kind] = jnp.zeros(total.shape[1:], jnp.float32)
                own_scale[kind] = jnp.broadcast_to(inverse_length(own_block(1 - kind)), (rows, rows))
                return carry

            lax.fori_loop(0, 2, prepare, 0)

        def stage(step, carry):
            d = jnp.where(step == 0, reach, jnp.where(step == 1, 0, reach - step + 1))
            distance = turn - (d > 0).astype(jnp.int32)
            for kind in kinds:
                for sign in (1, -1):
                    z2, valid = position(kind, sign, distance)

                    @pl.when((d > 0) & valid & arrives(kind, d, z2))
                    def _():
                        await_block(kind, 2 * d + view(kind)[1], z2)
                        each(kind, arrival_sends(kind, d, z2), z2)

            def work(index, carry):
                kind = first_kind + ((index // 2) % 2) * (1 - 2 * first_kind)
                _, k, z = view(kind)
                source_k = (k + index // 4) % 2
                z2, valid = position(kind, 1 - 2 * (index % 2), distance)
                slot = 2 * d + source_k

                @pl.when(valid & need(k, z, d, source_k, z2))
                def _():
                    @pl.when(source_k != k)
                    def _():
                        await_block(kind, slot, z2)

                    tile(kind, slot, z2)

                return carry

            return lax.fori_loop(0, 8, work, carry)

        return lax.fori_loop(0, reach + 1, stage, carry)

    lax.fori_loop(0, depth + 1, advance, 0)

    for kind, out in ((0, image_out), (1, text_out)):
        scale = own_scale[kind][:, :1]
        unit = own_block(1 - kind).astype(jnp.float32) * scale
        grad = LOGIT_SCALE * total[kind]
        inner = jnp.sum(unit * grad, axis=-1, keepdims=True)
        out[...] = ((grad - unit * inner) * scale).astype(out.dtype)

    def settle(z2, carry):
        for kind in (0, 1):
            each(kind, own_sends(kind, z2), z2, finish=True)
            for d in range(1, reach + 1):
                @pl.when(arrives(kind, d, z2))
                def _():
                    each(kind, arrival_sends(kind, d, z2), z2, finish=True)
        return carry

    lax.fori_loop(0, depth, settle, 0)


def solution(mesh):
    cycle, depth = mesh.shape["blk"], mesh.shape["grp"]
    window = min(20, cycle * depth // 2)
    chips = cycle // 2
    reach = 1
    while (2 * reach + 1) * depth - (depth - 1) < window:
        reach += 1
    slots = 2 * (reach + 1)

    def per_device(image_embeds, text_embeds):
        rows, width = image_embeds.shape
        shape = jax.ShapeDtypeStruct((rows, width), jnp.bfloat16)
        return pl.pallas_call(
            functools.partial(kernel, chips, depth, reach, window),
            out_shape=(shape, shape),
            in_specs=[pl.BlockSpec(memory_space=pl.ANY)] * 2,
            out_specs=(pl.BlockSpec(memory_space=pltpu.VMEM),) * 2,
            scratch_shapes=[
                pltpu.VMEM((2, slots, depth, rows, width), jnp.bfloat16),
                pltpu.VMEM((2, rows, width), jnp.float32),
                pltpu.VMEM((2, rows, rows), jnp.float32),
                pltpu.SemaphoreType.DMA((2,)),
                pltpu.SemaphoreType.DMA((2, 6 + 2 * reach, depth)),
                pltpu.SemaphoreType.DMA((2, slots, depth)),
            ],
            compiler_params=pltpu.CompilerParams(collective_id=0, has_side_effects=True),
        )(image_embeds, text_embeds)

    placed = P(("blk", "grp"), None)
    return jax.shard_map(
        per_device, mesh=mesh, in_specs=(placed, placed), out_specs=(placed, placed), check_vma=False
    )
```

```python
import functools

import jax
import jax.numpy as jnp
from jax import lax
from jax.experimental import pallas as pl
from jax.experimental.pallas import tpu as pltpu
from jax.sharding import PartitionSpec as P

LOGIT_SCALE = 10.0
BIAS_LOGIT = -2.0
EPSILON = 1e-06
MESH = pl.DeviceIdType.MESH


def kernel(chips, depth, reach, window, image_ref, text_ref, image_out, text_out,
           held, total, own_scale, local_sem, send_sem, recv_sem):
    blk = lax.axis_index("blk")
    grp = lax.axis_index("grp")
    chip, core = blk // 2, blk % 2
    relayed = chips == 4 and reach == 2 and 4 * depth - 1 < window

    def view(kind):
        return (
            chip + kind * (chips - 1 - 2 * chip),
            core + kind * (1 - 2 * core),
            grp + kind * (depth - 1 - 2 * grp),
        )

    def device(kind, c, k, z):
        c = (c + chips) % chips
        linear = 2 * c + k
        return (
            linear + kind * (2 * chips - 1 - 2 * linear),
            z + kind * (depth - 1 - 2 * z),
        )

    first_kind = 1 - chip % 2 if relayed else 0
    kinds = (first_kind, 1 - first_kind)

    def need(k, z, d, source_k, source_z):
        offset = (2 * d + k - source_k) * depth + z - source_z
        return (offset >= 0) & (offset < window)

    def chip_need(z, d, source_k, source_z):
        return need(0, z, d, source_k, source_z) | need(1, z, d, source_k, source_z)

    def arrives(kind, d, source_z):
        c, k, z = view(kind)
        wanted = chip_need(z, d, k, source_z)
        if relayed:
            wanted = wanted | ((d == 2) & (c % 2 == 1))
        return wanted

    def copy(kind, path, source_slot, target_slot, z, target):
        return pltpu.make_async_remote_copy(
            src_ref=held.at[kind, source_slot, z],
            dst_ref=held.at[kind, target_slot, z],
            send_sem=send_sem.at[kind, path, z],
            recv_sem=recv_sem.at[kind, target_slot, z],
            device_id=target,
            device_id_type=MESH,
        )

    def own_sends(kind, z2):
        c, k, z = view(kind)
        sends = [
            ((z2 <= z) & (z + 1 < depth), 0, k, k, (c, k, z + 1)),
            ((z2 >= z) & (z >= 1), 1, k, k, (c, k, z - 1)),
        ]
        for d in range(1, reach + 1):
            wanted = chip_need(z, d, k, z2)
            if relayed and d == 1:
                inside = (z2 > 0) & (z2 < depth - 1)
                wanted = (c % 2 == 0) & (inside | (z2 == z))
            if relayed and d == 2:
                wanted = wanted | (c % 2 == 1)
            sends.append((wanted, 1 + d, k, 2 * d + k, (c + d, k, z)))
        sends.append((need(1 - k, z, 0, k, z2), 2 + reach, k, k, (c, 1 - k, z)))
        return sends

    def arrival_sends(kind, d, z2):
        c, k, z = view(kind)
        sends = []
        slot = 2 * d + k
        if relayed:
            sends.append(((c % 2 == 1) & (d == 2), 3 + reach, slot, 2 + k, (c - 1, k, z)))
            outer = (c % 2 == 1) & (d == 1) & ((z2 == 0) | (z2 == depth - 1))
            sends.append((outer & (z2 <= z) & (z + 1 < depth),
                          4 + 2 * reach, slot, slot, (c, k, z + 1)))
            sends.append((outer & (z2 >= z) & (z >= 1),
                          5 + 2 * reach, slot, slot, (c, k, z - 1)))
        sends.append((need(1 - k, z, d, k, z2), 3 + reach + d, slot, slot, (c, 1 - k, z)))
        return sends

    def each(kind, sends, z2, finish=False):
        for wanted, path, source_slot, target_slot, target in sends:
            @pl.when(wanted)
            def _():
                moved = copy(kind, path, source_slot, target_slot, z2, device(kind, *target))
                if finish:
                    moved.wait_send()
                else:
                    moved.start()

    def await_block(kind, slot, z2):
        c, k, z = view(kind)
        copy(kind, 0, slot, slot, z2, device(kind, c, 1 - k, z)).wait_recv()

    own = []
    for kind, ref in ((0, text_ref), (1, image_ref)):
        _, k, z = view(kind)
        loaded = pltpu.make_async_copy(ref, held.at[kind, k, z], local_sem.at[kind])
        loaded.start()
        own.append(loaded)

    barrier = pltpu.get_barrier_semaphore()

    def greet(target):
        pl.semaphore_signal(barrier, inc=1, device_id=target, device_id_type=MESH)

    greet((2 * chip + 1 - core, grp))
    if relayed:
        partners = [chip + 1 - 2 * (chip % 2), (chip + 2) % 4]
    else:
        partners = [(chip + d + chips) % chips for d in range(-reach, reach + 1) if d]
    for partner in partners:
        greet((2 * partner + core, grp))

    @pl.when(grp > 0)
    def _():
        greet((blk, grp - 1))

    @pl.when(grp < depth - 1)
    def _():
        greet((blk, grp + 1))

    for loaded in own:
        loaded.wait()
    pl.semaphore_wait(
        barrier,
        1 + len(partners) + (grp > 0).astype(jnp.int32) + (grp < depth - 1).astype(jnp.int32),
    )

    def own_block(kind):
        _, k, z = view(kind)
        return held[kind, k, z]

    def inverse_length(block):
        wide = block.astype(jnp.float32)
        return lax.rsqrt(jnp.sum(wide * wide, axis=-1, keepdims=True) + EPSILON)

    rows = held.shape[3]

    def tile(kind, slot, z2):
        _, k, z = view(kind)
        other = held[kind, slot, z2]
        mine = own_block(1 - kind)
        columns = jnp.broadcast_to(inverse_length(other), (rows, rows)).T
        product = lax.dot_general(
            mine, other, (((1,), (1,)), ((), ())), preferred_element_type=jnp.float32
        )
        logits = LOGIT_SCALE * product * own_scale[kind] * columns + BIAS_LOGIT
        inverse = jnp.exp(-logits)
        weights = 1.0 / (1.0 + inverse)
        diagonal = lax.broadcasted_iota(jnp.int32, (rows, rows), 0) == lax.broadcasted_iota(
            jnp.int32, (rows, rows), 1
        )
        first = ((slot == k) & (z2 == z)).astype(jnp.float32)
        positive = jnp.where(diagonal, first, 0.0)
        weights = jnp.where(positive > 0.5, -inverse * weights, weights)
        scaled = (weights * columns).astype(jnp.bfloat16)
        total[kind] += jnp.dot(scaled, other, preferred_element_type=jnp.float32)

    def position(kind, sign, distance):
        _, _, z = view(kind)
        z2 = z + sign * distance
        valid = (z2 >= 0) & (z2 < depth) & (distance >= 0)
        return z2, valid & ((sign > 0) | (distance > 0))

    def prepare(kind, carry):
        total[kind] = jnp.zeros(total.shape[1:], jnp.float32)
        own_scale[kind] = jnp.broadcast_to(inverse_length(own_block(1 - kind)), (rows, rows))
        return carry

    def start_own(kind):
        _, _, z = view(kind)
        each(kind, own_sends(kind, z), z)

    for kind in kinds:
        start_own(kind)
    lax.fori_loop(0, 2, prepare, 0)

    def half_turn(index, carry):
        turn = index // 2
        kind = first_kind + (index % 2) * (1 - 2 * first_kind)
        _, k, z = view(kind)

        for sign in (1, -1):
            z2, valid = position(kind, sign, turn)

            @pl.when(valid & (turn > 0))
            def _():
                await_block(kind, k, z2)
                each(kind, own_sends(kind, z2), z2)

        def stage(step, carry):
            d = jnp.where(step == 0, reach, jnp.where(step == 1, 0, reach - step + 1))
            distance = turn - (d > 0).astype(jnp.int32)
            for sign in (1, -1):
                z2, valid = position(kind, sign, distance)

                @pl.when((d > 0) & valid & arrives(kind, d, z2))
                def _():
                    await_block(kind, 2 * d + k, z2)
                    each(kind, arrival_sends(kind, d, z2), z2)

            def work(item, carry):
                source_k = (k + item // 2) % 2
                z2, valid = position(kind, 1 - 2 * (item % 2), distance)
                slot = 2 * d + source_k

                @pl.when(valid & need(k, z, d, source_k, z2))
                def _():
                    @pl.when(source_k != k)
                    def _():
                        await_block(kind, slot, z2)

                    tile(kind, slot, z2)

                return carry

            return lax.fori_loop(0, 4, work, carry)

        return lax.fori_loop(0, reach + 1, stage, carry)

    lax.fori_loop(0, 2 * (depth + 1), half_turn, 0)

    for kind, out in ((0, image_out), (1, text_out)):
        scale = own_scale[kind][:, :1]
        unit = own_block(1 - kind).astype(jnp.float32) * scale
        grad = LOGIT_SCALE * total[kind]
        inner = jnp.sum(unit * grad, axis=-1, keepdims=True)
        out[...] = ((grad - unit * inner) * scale).astype(out.dtype)

    def settle(z2, carry):
        for kind in (0, 1):
            each(kind, own_sends(kind, z2), z2, finish=True)
            for d in range(1, reach + 1):
                @pl.when(arrives(kind, d, z2))
                def _():
                    each(kind, arrival_sends(kind, d, z2), z2, finish=True)
        return carry

    lax.fori_loop(0, depth, settle, 0)


def solution(mesh):
    cycle, depth = mesh.shape["blk"], mesh.shape["grp"]
    window = min(20, cycle * depth // 2)
    chips = cycle // 2
    reach = 1
    while (2 * reach + 1) * depth - (depth - 1) < window:
        reach += 1
    slots = 2 * (reach + 1)

    def per_device(image_embeds, text_embeds):
        rows, width = image_embeds.shape
        shape = jax.ShapeDtypeStruct((rows, width), jnp.bfloat16)
        return pl.pallas_call(
            functools.partial(kernel, chips, depth, reach, window),
            out_shape=(shape, shape),
            in_specs=[pl.BlockSpec(memory_space=pl.ANY)] * 2,
            out_specs=(pl.BlockSpec(memory_space=pltpu.VMEM),) * 2,
            scratch_shapes=[
                pltpu.VMEM((2, slots, depth, rows, width), jnp.bfloat16),
                pltpu.VMEM((2, rows, width), jnp.float32),
                pltpu.VMEM((2, rows, rows), jnp.float32),
                pltpu.SemaphoreType.DMA((2,)),
                pltpu.SemaphoreType.DMA((2, 6 + 2 * reach, depth)),
                pltpu.SemaphoreType.DMA((2, slots, depth)),
            ],
            compiler_params=pltpu.CompilerParams(collective_id=0, has_side_effects=True),
        )(image_embeds, text_embeds)

    placed = P(("blk", "grp"), None)
    return jax.shard_map(
        per_device, mesh=mesh, in_specs=(placed, placed), out_specs=(placed, placed), check_vma=False
    )
```

```python
import functools

import jax
import jax.numpy as jnp
from jax import lax
from jax.experimental import pallas as pl
from jax.experimental.pallas import tpu as pltpu
from jax.sharding import PartitionSpec as P

LOGIT_SCALE = 10.0
BIAS_LOGIT = -2.0
EPSILON = 1e-06
MESH = pl.DeviceIdType.MESH


def kernel(chips, depth, reach, window, image_ref, text_ref, image_out, text_out,
           held, total, own_scale, local_sem, send_sem, recv_sem):
    blk = lax.axis_index("blk")
    grp = lax.axis_index("grp")
    chip, core = blk // 2, blk % 2
    relayed = chips == 4 and reach == 2 and 4 * depth - 1 < window

    def view(kind):
        return (
            chip + kind * (chips - 1 - 2 * chip),
            core + kind * (1 - 2 * core),
            grp + kind * (depth - 1 - 2 * grp),
        )

    def device(kind, c, k, z):
        c = (c + chips) % chips
        linear = 2 * c + k
        return (
            linear + kind * (2 * chips - 1 - 2 * linear),
            z + kind * (depth - 1 - 2 * z),
        )

    first_kind = 1 - chip % 2 if relayed else 0
    kinds = (first_kind, 1 - first_kind)

    def need(k, z, d, source_k, source_z):
        offset = (2 * d + k - source_k) * depth + z - source_z
        return (offset >= 0) & (offset < window)

    def chip_need(z, d, source_k, source_z):
        return need(0, z, d, source_k, source_z) | need(1, z, d, source_k, source_z)

    def arrives(kind, d, source_z):
        c, k, z = view(kind)
        wanted = chip_need(z, d, k, source_z)
        if relayed:
            wanted = wanted | ((d == 2) & (c % 2 == 1))
        return wanted

    def copy(kind, path, source_slot, target_slot, z, target):
        return pltpu.make_async_remote_copy(
            src_ref=held.at[kind, source_slot, z],
            dst_ref=held.at[kind, target_slot, z],
            send_sem=send_sem.at[kind, path, z],
            recv_sem=recv_sem.at[kind, target_slot, z],
            device_id=target,
            device_id_type=MESH,
        )

    def own_sends(kind, z2):
        c, k, z = view(kind)
        sends = [
            ((z2 <= z) & (z + 1 < depth), 0, k, k, (c, k, z + 1)),
            ((z2 >= z) & (z >= 1), 1, k, k, (c, k, z - 1)),
        ]
        for d in range(1, reach + 1):
            wanted = chip_need(z, d, k, z2)
            if relayed and d == 1:
                wanted = c % 2 == 0
            if relayed and d == 2:
                wanted = wanted | (c % 2 == 1)
            sends.append((wanted, 1 + d, k, 2 * d + k, (c + d, k, z)))
        sends.append((need(1 - k, z, 0, k, z2), 2 + reach, k, k, (c, 1 - k, z)))
        return sends

    def arrival_sends(kind, d, z2):
        c, k, z = view(kind)
        sends = []
        slot = 2 * d + k
        if relayed:
            outer = (z2 == 0) | (z2 == depth - 1)
            crossing = (z2 == z) | jnp.logical_not(outer)
            sends.append(((c % 2 == 1) & (d == 2) & crossing,
                          3 + reach, slot, 2 + k, (c - 1, k, z)))
            outer = (c % 2 == 0) & (d == 1) & outer
            sends.append((outer & (z2 <= z) & (z + 1 < depth),
                          4 + 2 * reach, slot, slot, (c, k, z + 1)))
            sends.append((outer & (z2 >= z) & (z >= 1),
                          5 + 2 * reach, slot, slot, (c, k, z - 1)))
        sends.append((need(1 - k, z, d, k, z2), 3 + reach + d, slot, slot, (c, 1 - k, z)))
        return sends

    def each(kind, sends, z2, finish=False):
        for wanted, path, source_slot, target_slot, target in sends:
            @pl.when(wanted)
            def _():
                moved = copy(kind, path, source_slot, target_slot, z2, device(kind, *target))
                if finish:
                    moved.wait_send()
                else:
                    moved.start()

    def await_block(kind, slot, z2):
        c, k, z = view(kind)
        copy(kind, 0, slot, slot, z2, device(kind, c, 1 - k, z)).wait_recv()

    own = []
    for kind, ref in ((0, text_ref), (1, image_ref)):
        _, k, z = view(kind)
        loaded = pltpu.make_async_copy(ref, held.at[kind, k, z], local_sem.at[kind])
        loaded.start()
        own.append(loaded)

    barrier = pltpu.get_barrier_semaphore()

    def greet(target):
        pl.semaphore_signal(barrier, inc=1, device_id=target, device_id_type=MESH)

    greet((2 * chip + 1 - core, grp))
    if relayed:
        partners = [chip + 1 - 2 * (chip % 2), (chip + 2) % 4]
    else:
        partners = [(chip + d + chips) % chips for d in range(-reach, reach + 1) if d]
    for partner in partners:
        greet((2 * partner + core, grp))

    @pl.when(grp > 0)
    def _():
        greet((blk, grp - 1))

    @pl.when(grp < depth - 1)
    def _():
        greet((blk, grp + 1))

    for loaded in own:
        loaded.wait()
    pl.semaphore_wait(
        barrier,
        1 + len(partners) + (grp > 0).astype(jnp.int32) + (grp < depth - 1).astype(jnp.int32),
    )

    def own_block(kind):
        _, k, z = view(kind)
        return held[kind, k, z]

    def inverse_length(block):
        wide = block.astype(jnp.float32)
        return lax.rsqrt(jnp.sum(wide * wide, axis=-1, keepdims=True) + EPSILON)

    rows = held.shape[3]

    def tile(kind, slot, z2):
        _, k, z = view(kind)
        other = held[kind, slot, z2]
        mine = own_block(1 - kind)
        columns = jnp.broadcast_to(inverse_length(other), (rows, rows)).T
        product = lax.dot_general(
            mine, other, (((1,), (1,)), ((), ())), preferred_element_type=jnp.float32
        )
        logits = LOGIT_SCALE * product * own_scale[kind] * columns + BIAS_LOGIT
        inverse = jnp.exp(-logits)
        weights = 1.0 / (1.0 + inverse)
        diagonal = lax.broadcasted_iota(jnp.int32, (rows, rows), 0) == lax.broadcasted_iota(
            jnp.int32, (rows, rows), 1
        )
        first = ((slot == k) & (z2 == z)).astype(jnp.float32)
        positive = jnp.where(diagonal, first, 0.0)
        weights = jnp.where(positive > 0.5, -inverse * weights, weights)
        scaled = (weights * columns).astype(jnp.bfloat16)
        total[kind] += jnp.dot(scaled, other, preferred_element_type=jnp.float32)

    def position(kind, sign, distance):
        _, _, z = view(kind)
        z2 = z + sign * distance
        valid = (z2 >= 0) & (z2 < depth) & (distance >= 0)
        return z2, valid & ((sign > 0) | (distance > 0))

    def prepare(kind, carry):
        total[kind] = jnp.zeros(total.shape[1:], jnp.float32)
        own_scale[kind] = jnp.broadcast_to(inverse_length(own_block(1 - kind)), (rows, rows))
        return carry

    def start_own(kind):
        _, _, z = view(kind)
        each(kind, own_sends(kind, z), z)

    for kind in kinds:
        start_own(kind)
    lax.fori_loop(0, 2, prepare, 0)

    steps = reach + 1

    def advance(index, carry):
        turn, part = index // (2 * steps), index % (2 * steps)
        which, step = part // steps, part % steps
        d = jnp.where(step == 0, reach, jnp.where(step == 1, 0, reach - step + 1))
        opens = step == 0
        receives = d > 0
        computes = index >= 0
        if relayed:
            last = turn == depth
            far = (part == 0) | (part == 3) | (part == 5)
            which = jnp.where(last, part % 2, which)
            d = jnp.where(last, jnp.where(far, 2, 1), d)
            receives = jnp.where(last, part < 4, receives)
            computes = jnp.logical_not(last & ((part == 2) | (part == 3)))
        kind = first_kind + which * (1 - 2 * first_kind)
        _, k, z = view(kind)
        distance = turn - (d > 0).astype(jnp.int32)

        for sign in (1, -1):
            z2, valid = position(kind, sign, turn)

            @pl.when(valid & opens & (turn > 0))
            def _():
                await_block(kind, k, z2)
                each(kind, own_sends(kind, z2), z2)

        for sign in (1, -1):
            z2, valid = position(kind, sign, distance)

            @pl.when(receives & valid & arrives(kind, d, z2))
            def _():
                await_block(kind, 2 * d + k, z2)
                each(kind, arrival_sends(kind, d, z2), z2)

        def work(item, carry):
            source_k = (k + item // 2) % 2
            z2, valid = position(kind, 1 - 2 * (item % 2), distance)
            slot = 2 * d + source_k

            @pl.when(valid & computes & need(k, z, d, source_k, z2))
            def _():
                @pl.when(source_k != k)
                def _():
                    await_block(kind, slot, z2)

                tile(kind, slot, z2)

            return carry

        return lax.fori_loop(0, 4, work, carry)

    lax.fori_loop(0, 2 * steps * (depth + 1), advance, 0)

    for kind, out in ((0, image_out), (1, text_out)):
        scale = own_scale[kind][:, :1]
        unit = own_block(1 - kind).astype(jnp.float32) * scale
        grad = LOGIT_SCALE * total[kind]
        inner = jnp.sum(unit * grad, axis=-1, keepdims=True)
        out[...] = ((grad - unit * inner) * scale).astype(out.dtype)

    def settle(z2, carry):
        for kind in (0, 1):
            each(kind, own_sends(kind, z2), z2, finish=True)
            for d in range(1, reach + 1):
                @pl.when(arrives(kind, d, z2))
                def _():
                    each(kind, arrival_sends(kind, d, z2), z2, finish=True)
        return carry

    lax.fori_loop(0, depth, settle, 0)


def solution(mesh):
    cycle, depth = mesh.shape["blk"], mesh.shape["grp"]
    window = min(20, cycle * depth // 2)
    chips = cycle // 2
    reach = 1
    while (2 * reach + 1) * depth - (depth - 1) < window:
        reach += 1
    slots = 2 * (reach + 1)

    def per_device(image_embeds, text_embeds):
        rows, width = image_embeds.shape
        shape = jax.ShapeDtypeStruct((rows, width), jnp.bfloat16)
        return pl.pallas_call(
            functools.partial(kernel, chips, depth, reach, window),
            out_shape=(shape, shape),
            in_specs=[pl.BlockSpec(memory_space=pl.ANY)] * 2,
            out_specs=(pl.BlockSpec(memory_space=pltpu.VMEM),) * 2,
            scratch_shapes=[
                pltpu.VMEM((2, slots, depth, rows, width), jnp.bfloat16),
                pltpu.VMEM((2, rows, width), jnp.float32),
                pltpu.VMEM((2, rows, rows), jnp.float32),
                pltpu.SemaphoreType.DMA((2,)),
                pltpu.SemaphoreType.DMA((2, 6 + 2 * reach, depth)),
                pltpu.SemaphoreType.DMA((2, slots, depth)),
            ],
            compiler_params=pltpu.CompilerParams(collective_id=0, has_side_effects=True),
        )(image_embeds, text_embeds)

    placed = P(("blk", "grp"), None)
    return jax.shard_map(
        per_device, mesh=mesh, in_specs=(placed, placed), out_specs=(placed, placed), check_vma=False
    )
```

```python
import functools

import jax
import jax.numpy as jnp
from jax import lax
from jax.experimental import pallas as pl
from jax.experimental.pallas import tpu as pltpu
from jax.sharding import PartitionSpec as P

LOGIT_SCALE = 10.0
BIAS_LOGIT = -2.0
EPSILON = 1e-06
MESH = pl.DeviceIdType.MESH


def kernel(chips, depth, reach, window, image_ref, text_ref, image_out, text_out,
           held, total, own_scale, local_sem, send_sem, recv_sem):
    blk = lax.axis_index("blk")
    grp = lax.axis_index("grp")
    chip, core = blk // 2, blk % 2
    relayed = chips == 4 and reach == 2 and 4 * depth - 1 < window

    def view(kind):
        return (
            chip + kind * (chips - 1 - 2 * chip),
            core + kind * (1 - 2 * core),
            grp + kind * (depth - 1 - 2 * grp),
        )

    def device(kind, c, k, z):
        c = (c + chips) % chips
        linear = 2 * c + k
        return (
            linear + kind * (2 * chips - 1 - 2 * linear),
            z + kind * (depth - 1 - 2 * z),
        )

    first_kind = 1 - chip % 2 if relayed else 0
    kinds = (first_kind, 1 - first_kind)

    def need(k, z, d, source_k, source_z):
        offset = (2 * d + k - source_k) * depth + z - source_z
        return (offset >= 0) & (offset < window)

    def chip_need(z, d, source_k, source_z):
        return need(0, z, d, source_k, source_z) | need(1, z, d, source_k, source_z)

    def arrives(kind, d, source_z):
        c, k, z = view(kind)
        wanted = chip_need(z, d, k, source_z)
        if relayed:
            wanted = wanted | ((d == 2) & (c % 2 == 1))
        return wanted

    def copy(kind, path, source_slot, target_slot, z, target):
        return pltpu.make_async_remote_copy(
            src_ref=held.at[kind, source_slot, z],
            dst_ref=held.at[kind, target_slot, z],
            send_sem=send_sem.at[kind, path, z],
            recv_sem=recv_sem.at[kind, target_slot, z],
            device_id=target,
            device_id_type=MESH,
        )

    def own_sends(kind, z2):
        c, k, z = view(kind)
        sends = [
            ((z2 <= z) & (z + 1 < depth), 0, k, k, (c, k, z + 1)),
            ((z2 >= z) & (z >= 1), 1, k, k, (c, k, z - 1)),
        ]
        for d in range(1, reach + 1):
            wanted = chip_need(z, d, k, z2)
            if relayed and d == 1:
                inside = (z2 > 0) & (z2 < depth - 1)
                wanted = (c % 2 == 0) & (inside | (z2 == z))
            if relayed and d == 2:
                wanted = wanted | (c % 2 == 1)
            sends.append((wanted, 1 + d, k, 2 * d + k, (c + d, k, z)))
        sends.append((need(1 - k, z, 0, k, z2), 2 + reach, k, k, (c, 1 - k, z)))
        return sends

    def arrival_sends(kind, d, z2):
        c, k, z = view(kind)
        sends = []
        slot = 2 * d + k
        if relayed:
            sends.append(((c % 2 == 1) & (d == 2), 3 + reach, slot, 2 + k, (c - 1, k, z)))
            outer = (c % 2 == 1) & (d == 1) & ((z2 == 0) | (z2 == depth - 1))
            sends.append((outer & (z2 <= z) & (z + 1 < depth),
                          4 + 2 * reach, slot, slot, (c, k, z + 1)))
            sends.append((outer & (z2 >= z) & (z >= 1),
                          5 + 2 * reach, slot, slot, (c, k, z - 1)))
        sends.append((need(1 - k, z, d, k, z2), 3 + reach + d, slot, slot, (c, 1 - k, z)))
        return sends

    def each(kind, sends, z2, finish=False):
        for wanted, path, source_slot, target_slot, target in sends:
            @pl.when(wanted)
            def _():
                moved = copy(kind, path, source_slot, target_slot, z2, device(kind, *target))
                if finish:
                    moved.wait_send()
                else:
                    moved.start()

    def await_block(kind, slot, z2):
        c, k, z = view(kind)
        copy(kind, 0, slot, slot, z2, device(kind, c, 1 - k, z)).wait_recv()

    own = []
    for kind, ref in ((0, text_ref), (1, image_ref)):
        _, k, z = view(kind)
        loaded = pltpu.make_async_copy(ref, held.at[kind, k, z], local_sem.at[kind])
        loaded.start()
        own.append(loaded)

    barrier = pltpu.get_barrier_semaphore()

    def greet(target):
        pl.semaphore_signal(barrier, inc=1, device_id=target, device_id_type=MESH)

    greet((2 * chip + 1 - core, grp))
    if relayed:
        partners = [chip + 1 - 2 * (chip % 2), (chip + 2) % 4]
    else:
        partners = [(chip + d + chips) % chips for d in range(-reach, reach + 1) if d]
    for partner in partners:
        greet((2 * partner + core, grp))

    @pl.when(grp > 0)
    def _():
        greet((blk, grp - 1))

    @pl.when(grp < depth - 1)
    def _():
        greet((blk, grp + 1))

    for loaded in own:
        loaded.wait()
    pl.semaphore_wait(
        barrier,
        1 + len(partners) + (grp > 0).astype(jnp.int32) + (grp < depth - 1).astype(jnp.int32),
    )

    def own_block(kind):
        _, k, z = view(kind)
        return held[kind, k, z]

    def inverse_length(block):
        wide = block.astype(jnp.float32)
        return lax.rsqrt(jnp.sum(wide * wide, axis=-1, keepdims=True) + EPSILON)

    rows = held.shape[3]

    def tile(kind, slot, z2):
        _, k, z = view(kind)
        other = held[kind, slot, z2]
        mine = own_block(1 - kind)
        columns = jnp.broadcast_to(inverse_length(other), (rows, rows)).T
        product = lax.dot_general(
            mine, other, (((1,), (1,)), ((), ())), preferred_element_type=jnp.float32
        )
        logits = LOGIT_SCALE * product * own_scale[kind] * columns + BIAS_LOGIT
        inverse = jnp.exp(-logits)
        weights = 1.0 / (1.0 + inverse)
        diagonal = lax.broadcasted_iota(jnp.int32, (rows, rows), 0) == lax.broadcasted_iota(
            jnp.int32, (rows, rows), 1
        )
        first = ((slot == k) & (z2 == z)).astype(jnp.float32)
        positive = jnp.where(diagonal, first, 0.0)
        weights = jnp.where(positive > 0.5, -inverse * weights, weights)
        scaled = (weights * columns).astype(jnp.bfloat16)
        total[kind] += jnp.dot(scaled, other, preferred_element_type=jnp.float32)

    def position(kind, sign, distance):
        _, _, z = view(kind)
        z2 = z + sign * distance
        valid = (z2 >= 0) & (z2 < depth) & (distance >= 0)
        return z2, valid & ((sign > 0) | (distance > 0))

    def prepare(kind, carry):
        total[kind] = jnp.zeros(total.shape[1:], jnp.float32)
        own_scale[kind] = jnp.broadcast_to(inverse_length(own_block(1 - kind)), (rows, rows))
        return carry

    def start_own(kind):
        _, _, z = view(kind)
        each(kind, own_sends(kind, z), z)

    for kind in kinds:
        start_own(kind)
    lax.fori_loop(0, 2, prepare, 0)

    steps = reach + 1

    def advance(index, carry):
        turn, part = index // (2 * steps), index % (2 * steps)
        which, step = part // steps, part % steps
        d = jnp.where(step == 0, reach, jnp.where(step == 1, 0, reach - step + 1))
        opens = step == 0
        receives = d > 0
        computes = index >= 0
        if relayed:
            last = turn == depth
            far = (part == 0) | (part == 2) | (part == 4)
            which = jnp.where(last, ((part == 2) | (part >= 4)).astype(jnp.int32), which)
            d = jnp.where(last, jnp.where(far, 2, 1), d)
            receives = jnp.where(last, (part < 3) | (part == 5), receives)
            computes = jnp.logical_not(last & ((part == 1) | (part == 2)))
        kind = first_kind + which * (1 - 2 * first_kind)
        _, k, z = view(kind)
        distance = turn - (d > 0).astype(jnp.int32)

        for sign in (1, -1):
            z2, valid = position(kind, sign, turn)

            @pl.when(valid & opens & (turn > 0))
            def _():
                await_block(kind, k, z2)
                each(kind, own_sends(kind, z2), z2)

        for sign in (1, -1):
            z2, valid = position(kind, sign, distance)

            @pl.when(receives & valid & arrives(kind, d, z2))
            def _():
                await_block(kind, 2 * d + k, z2)
                each(kind, arrival_sends(kind, d, z2), z2)

        def work(item, carry):
            source_k = (k + item // 2) % 2
            z2, valid = position(kind, 1 - 2 * (item % 2), distance)
            slot = 2 * d + source_k

            @pl.when(valid & computes & need(k, z, d, source_k, z2))
            def _():
                @pl.when(source_k != k)
                def _():
                    await_block(kind, slot, z2)

                tile(kind, slot, z2)

            return carry

        return lax.fori_loop(0, 4, work, carry)

    lax.fori_loop(0, 2 * steps * (depth + 1), advance, 0)

    for kind, out in ((0, image_out), (1, text_out)):
        scale = own_scale[kind][:, :1]
        unit = own_block(1 - kind).astype(jnp.float32) * scale
        grad = LOGIT_SCALE * total[kind]
        inner = jnp.sum(unit * grad, axis=-1, keepdims=True)
        out[...] = ((grad - unit * inner) * scale).astype(out.dtype)

    def settle(z2, carry):
        for kind in (0, 1):
            each(kind, own_sends(kind, z2), z2, finish=True)
            for d in range(1, reach + 1):
                @pl.when(arrives(kind, d, z2))
                def _():
                    each(kind, arrival_sends(kind, d, z2), z2, finish=True)
        return carry

    lax.fori_loop(0, depth, settle, 0)


def solution(mesh):
    cycle, depth = mesh.shape["blk"], mesh.shape["grp"]
    window = min(20, cycle * depth // 2)
    chips = cycle // 2
    reach = 1
    while (2 * reach + 1) * depth - (depth - 1) < window:
        reach += 1
    slots = 2 * (reach + 1)

    def per_device(image_embeds, text_embeds):
        rows, width = image_embeds.shape
        shape = jax.ShapeDtypeStruct((rows, width), jnp.bfloat16)
        return pl.pallas_call(
            functools.partial(kernel, chips, depth, reach, window),
            out_shape=(shape, shape),
            in_specs=[pl.BlockSpec(memory_space=pl.ANY)] * 2,
            out_specs=(pl.BlockSpec(memory_space=pltpu.VMEM),) * 2,
            scratch_shapes=[
                pltpu.VMEM((2, slots, depth, rows, width), jnp.bfloat16),
                pltpu.VMEM((2, rows, width), jnp.float32),
                pltpu.VMEM((2, rows, rows), jnp.float32),
                pltpu.SemaphoreType.DMA((2,)),
                pltpu.SemaphoreType.DMA((2, 6 + 2 * reach, depth)),
                pltpu.SemaphoreType.DMA((2, slots, depth)),
            ],
            compiler_params=pltpu.CompilerParams(collective_id=0, has_side_effects=True),
        )(image_embeds, text_embeds)

    placed = P(("blk", "grp"), None)
    return jax.shard_map(
        per_device, mesh=mesh, in_specs=(placed, placed), out_specs=(placed, placed), check_vma=False
    )
```
